32 devices in a mesh: shard: 8 (over z, y), tp: 4 (over x, core).
Axes of the slice: x: 2, y: 2, z: 4, core: 2. Of those that a mesh axis runs over, the one named last changes fastest.
Arguments:
- gradient: bfloat16 [4096, 16384], P('shard', 'tp'), may hold values from -2 to 2
- table: int32 [256, 3], replicated, may hold values from 0 to 31, as said below
- left_stat: bfloat16 [384, 512, 512], P(('shard', 'tp')), as said below
- right_stat: bfloat16 [384, 512, 512], P(('shard', 'tp')), as said below
- left_basis: bfloat16 [384, 512, 512], P(('shard', 'tp')), may hold values from -0.25 to 0.25
- right_basis: bfloat16 [384, 512, 512], P(('shard', 'tp')), may hold values from -0.25 to 0.25
- moment: bfloat16 [384, 512, 512], P(('shard', 'tp')), may hold values from -2 to 2
- second: float32 [384, 512, 512], P(('shard', 'tp')), may hold values from 0.02 to 0.2
Outputs:
- update: bfloat16 [4096, 16384], P('shard', 'tp')
- new_left: bfloat16 [384, 512, 512], P(('shard', 'tp'))
- new_right: bfloat16 [384, 512, 512], P(('shard', 'tp'))
- new_moment: bfloat16 [384, 512, 512], P(('shard', 'tp'))
- new_second: float32 [384, 512, 512], P(('shard', 'tp'))
The draws below stay inside these ranges and needn't reach their ends.
Inputs may be any that keep to these rules, and one draw needn't show every extreme that they name: `table`: column 0 is a block row below 8, column 1 a block column below 32, column 2 an owner device below 32; every block appears in exactly one row; each device owns between 4 and 12 blocks, and some device owns exactly 12. `left_stat`: Symmetric. `right_stat`: Symmetric.
All inputs are finite; a program needn't handle non-finite values.
Results may differ from the reference program's by a relative error of at most 0.0085.
Values may be sent and summed in bfloat16 or wider, within the bound.
A program may use at most 192 MiB of HBM per device.

```python
import math
import jax
import jax.numpy as jnp
from jax import lax

ROWS = 4096
COLS = 16384
BLOCK = 512
NDEV = 32
NBR = 8
NBC = 32
NBLK = 256
OWN_MEAN = 8
SLOTS = 12


def stat_draw(key, salt):
    key = jax.random.fold_in(key, salt)
    first_key, second_key = jax.random.split(key)
    count = NDEV * SLOTS
    diagonal = jax.random.uniform(first_key, (count, BLOCK), jnp.float32, 1.0, 2.0)
    noise = jax.random.normal(second_key, (count, BLOCK, BLOCK), jnp.float32)
    symmetric = (noise + jnp.swapaxes(noise, 1, 2)) * (0.25 / jnp.sqrt(jnp.float32(BLOCK)))
    return symmetric + jnp.eye(BLOCK, dtype=jnp.float32)[None, :, :] * diagonal[:, None, :]


def draw_left_stat(key, part):
    return stat_draw(key, 11).astype(jnp.bfloat16)


def draw_right_stat(key, part):
    return stat_draw(key, 23).astype(jnp.bfloat16)


def draw_table(key, part):
    keys = jax.random.split(key, 4)
    reach = (OWN_MEAN + 1) // 2
    halfway = NDEV // 2
    shifts = jax.random.randint(keys[0], (halfway,), 0, reach + 1)
    shifts = shifts.at[0].set(reach)
    counts = jnp.concatenate([OWN_MEAN + shifts, OWN_MEAN - shifts])
    counts = counts[jax.random.permutation(keys[1], NDEV)]
    bounds = jnp.cumsum(counts)
    places = jnp.arange(NBLK, dtype=jnp.int32)
    owner_of = jnp.sum((bounds[None, :] <= places[:, None]).astype(jnp.int32), axis=1)
    blocks = jax.random.permutation(keys[2], NBLK).astype(jnp.int32)
    order = jax.random.permutation(keys[3], NBLK)
    owners = owner_of[order]
    return jnp.stack([blocks // NBC, blocks % NBC, owners], axis=1).astype(jnp.int32)


def level_of(key, extent, shards, low, top_value):
    level = 1.0
    for position, parts in shards:
        heights = jax.random.uniform(jax.random.fold_in(jax.random.fold_in(key, 6), position), (parts,), jnp.float32, low / len(shards), top_value / len(shards))
        level = level * jnp.repeat(jnp.exp(heights), extent[position] // parts).reshape((-1,) + (1,) * (len(extent) - 1 - position))
    return level


def gaussian(own_key, extent, width, bound, cuts=(), kind=jnp.bfloat16):
    level = level_of(own_key, extent, cuts, -0.22, 0.18) if cuts else 1.0
    array = jax.random.normal(own_key, extent, jnp.float32) * width * level
    return jnp.minimum(jnp.maximum(array, -bound), bound).astype(kind)


def setup_inputs(seed: int = 0) -> dict:
    arg_keys = jax.random.split(jax.random.key(seed), 9)
    return {
        "gradient": gaussian(arg_keys[0], (ROWS, COLS), 0.25, 2.0, ((0, 8), (1, 4))),
        "table": draw_table(jax.random.fold_in(arg_keys[8], 71), 0),
        "left_stat": draw_left_stat(jax.random.fold_in(arg_keys[8], 71), 0),
        "right_stat": draw_right_stat(jax.random.fold_in(arg_keys[8], 71), 0),
        "left_basis": gaussian(arg_keys[4], (NDEV * SLOTS, BLOCK, BLOCK), BLOCK ** -0.5, 0.25, ((0, 32),)),
        "right_basis": gaussian(arg_keys[5], (NDEV * SLOTS, BLOCK, BLOCK), BLOCK ** -0.5, 0.25, ((0, 32),)),
        "moment": gaussian(arg_keys[6], (NDEV * SLOTS, BLOCK, BLOCK), 0.25, 2.0, ((0, 32),)),
        "second": jnp.clip(jnp.exp(math.log(0.2) - 2.3025851 * jax.random.uniform(arg_keys[7], (NDEV * SLOTS, BLOCK, BLOCK), jnp.float32) ** level_of(arg_keys[7], (NDEV * SLOTS, BLOCK, BLOCK), ((0, 32),), -0.2, 0.2)), 0.02, 0.2),
    }


beta_moment = 0.9
beta_second = 0.95
beta_stats = 0.95
epsilon = 1e-08

def slot_table(table, slots):
    owners = table[:, 2]
    count = owners.shape[0]
    order = jnp.arange(count, dtype=jnp.int32)
    earlier = (owners[None, :] == owners[:, None]) & (order[None, :] < order[:, None])
    slot_rank = lax.optimization_barrier(jnp.sum(earlier.astype(jnp.int32), axis=1)).astype(jnp.int32)
    return (owners * slots + slot_rank).astype(jnp.int32)

def precondition(grad_block, left, right, left_q, right_q, first, squares):
    left_new = (beta_stats * left.astype(jnp.float32) + (1.0 - beta_stats) * jnp.dot(grad_block, grad_block.T, preferred_element_type=jnp.float32)).astype(jnp.bfloat16)
    right_new = (beta_stats * right.astype(jnp.float32) + (1.0 - beta_stats) * jnp.dot(grad_block.T, grad_block, preferred_element_type=jnp.float32)).astype(jnp.bfloat16)
    first_new = (beta_moment * first.astype(jnp.float32) + (1.0 - beta_moment) * grad_block.astype(jnp.float32)).astype(jnp.bfloat16)
    left_grad = jnp.dot(left_q.T, grad_block, preferred_element_type=jnp.float32).astype(jnp.bfloat16)
    rotated = jnp.dot(left_grad, right_q, preferred_element_type=jnp.float32)
    squares_new = beta_second * squares + (1.0 - beta_second) * rotated * rotated
    left_first = jnp.dot(left_q.T, first_new, preferred_element_type=jnp.float32).astype(jnp.bfloat16)
    first_rot = jnp.dot(left_first, right_q, preferred_element_type=jnp.float32)
    scaled = (first_rot / (jnp.sqrt(squares_new) + epsilon)).astype(jnp.bfloat16)
    back = jnp.dot(left_q, scaled, preferred_element_type=jnp.float32).astype(jnp.bfloat16)
    result = jnp.dot(back, right_q.T, preferred_element_type=jnp.float32).astype(jnp.bfloat16)
    return (result, left_new, right_new, first_new, squares_new)

def reference(gradient, table, left_stat, right_stat, left_basis, right_basis, moment, second):
    tiles = gradient.reshape(NBR, BLOCK, NBC, BLOCK).transpose(0, 2, 1, 3).reshape(NBLK, BLOCK, BLOCK)
    state_row = slot_table(table, SLOTS)
    block_id = (table[:, 0] * NBC + table[:, 1]).astype(jnp.int32)

    def one_block(index):
        slot = state_row[index]
        return precondition(tiles[block_id[index]], left_stat[slot], right_stat[slot], left_basis[slot], right_basis[slot], moment[slot], second[slot])
    results = lax.map(one_block, jnp.arange(NBLK, dtype=jnp.int32))
    block_updates, left_rows, right_rows, first_rows, square_rows = results
    new_left = left_stat.at[state_row].set(left_rows)
    new_right = right_stat.at[state_row].set(right_rows)
    new_moment = moment.at[state_row].set(first_rows)
    new_second = second.at[state_row].set(square_rows)
    placed = jnp.zeros((NBLK, BLOCK, BLOCK), jnp.bfloat16).at[block_id].set(block_updates)
    update = placed.reshape(NBR, NBC, BLOCK, BLOCK).transpose(0, 2, 1, 3).reshape(ROWS, COLS)
    return (update, new_left, new_right, new_moment, new_second)
```

```python
import functools

import jax
import jax.numpy as jnp
from jax import lax
from jax.experimental import pallas as pl
from jax.experimental.pallas import tpu as pltpu
from jax.sharding import PartitionSpec as P

beta_moment = 0.9
beta_second = 0.95
beta_stats = 0.95
epsilon = 1e-08
AXES = ("shard", "tp")


def slot_table(table, slots):
    owners = table[:, 2]
    count = owners.shape[0]
    order = jnp.arange(count, dtype=jnp.int32)
    earlier = (owners[None, :] == owners[:, None]) & (order[None, :] < order[:, None])
    slot_rank = jnp.sum(earlier.astype(jnp.int32), axis=1)
    return owners * slots + slot_rank


def exchange(array):
    return lax.all_to_all(array, AXES, split_axis=0, concat_axis=0, tiled=True)


def dot(a, b, dims):
    return lax.dot_general(a, b, (dims, ((), ())), preferred_element_type=jnp.float32)


def pack_kernel(group, slots, first, count, halves, tp_count, side, src_ref, col_ref, in_ref, out_ref):
    base = pl.program_id(0) * group

    def device(d, carry):
        for k in range(count):
            entry = (base + d) * slots + first + k
            src = src_ref[entry]
            col = pl.multiple_of(col_ref[entry] * side, side)
            for h in range(halves):
                out_ref[d, k, h] = in_ref[src + h * tp_count, :, pl.ds(col, side)]
        return carry

    lax.fori_loop(0, group, device, 0)


def pack(received, src, col, slots, first, count, halves, tp_count, side):
    dev_count, rows, cols = received.shape
    group = 4 if dev_count % 4 == 0 else 1
    return pl.pallas_call(
        functools.partial(pack_kernel, group, slots, first, count, halves, tp_count, side),
        grid_spec=pltpu.PrefetchScalarGridSpec(
            num_scalar_prefetch=2,
            grid=(dev_count // group,),
            in_specs=[pl.BlockSpec((dev_count, rows, cols), lambda i, *_: (0, 0, 0))],
            out_specs=pl.BlockSpec((group, count, halves, rows, side), lambda i, *_: (i, 0, 0, 0, 0)),
        ),
        out_shape=jax.ShapeDtypeStruct((dev_count, count, halves, rows, side), received.dtype),
        cost_estimate=pl.CostEstimate(flops=0, bytes_accessed=received.size * 6, transcendentals=0),
    )(src, col, received)


def unpack_kernel(group, firsts, halves, tp_count, cols_per_dev, side, own_ref, slot_ref, *refs):
    out_ref = refs[-1]
    base = pl.program_id(0) * group

    def device(d, carry):
        dev = base + d
        shard = dev // tp_count
        half = shard % halves
        place = (shard // halves * tp_count + dev % tp_count) * cols_per_dev
        for c in range(cols_per_dev):
            owner = own_ref[place + c]
            slot = slot_ref[place + c]
            value = refs[0][owner, jnp.minimum(slot, refs[0].shape[1] - 1), half]
            for ref, first in zip(refs[1:-1], firsts[1:]):
                inner = jnp.clip(slot - first, 0, ref.shape[1] - 1)
                value = jnp.where(slot >= first, ref[owner, inner, half], value)
            out_ref[d, :, c * side : (c + 1) * side] = value
        return carry

    lax.fori_loop(0, group, device, 0)


def unpack(chunks, firsts, own, slot, tp_count, cols_per_dev):
    dev_count, _, halves, rows, side = chunks[0].shape
    group = 4 if dev_count % 4 == 0 else 1
    cols = cols_per_dev * side
    return pl.pallas_call(
        functools.partial(unpack_kernel, group, firsts, halves, tp_count, cols_per_dev, side),
        grid_spec=pltpu.PrefetchScalarGridSpec(
            num_scalar_prefetch=2,
            grid=(dev_count // group,),
            in_specs=[pl.BlockSpec(c.shape, lambda i, *_: (0, 0, 0, 0, 0)) for c in chunks],
            out_specs=pl.BlockSpec((group, rows, cols), lambda i, *_: (i, 0, 0)),
        ),
        out_shape=jax.ShapeDtypeStruct((dev_count, rows, cols), chunks[0].dtype),
        cost_estimate=pl.CostEstimate(flops=0, bytes_accessed=dev_count * rows * cols * 5, transcendentals=0),
    )(own, slot, *chunks)


def slot_kernel(first, packed, mine_ref, x_ref, left, right, left_q, right_q, moment, second, *refs):
    out_ref, left_o, right_o, moment_o, second_o = refs[-5:]
    side = left.shape[-1]
    used = mine_ref[first + pl.program_id(0)] > 0

    @pl.when(used)
    def _():
        if packed:
            halves = x_ref.shape[2]
            parts = [x_ref[:, 0, h].reshape(side // halves, side) for h in range(halves)]
            grad = parts[0] if halves == 1 else jnp.concatenate(parts, axis=0)
        else:
            grad = x_ref[0]
        ql = left_q[0]
        qr = right_q[0]
        first_new = (
            beta_moment * moment[0].astype(jnp.float32)
            + (1.0 - beta_moment) * grad.astype(jnp.float32)
        ).astype(jnp.bfloat16)
        moment_o[0] = first_new
        left_grad = dot(ql, grad, ((0,), (0,))).astype(jnp.bfloat16)
        rotated = dot(left_grad, qr, ((1,), (0,)))
        squares_new = beta_second * second[0] + (1.0 - beta_second) * rotated * rotated
        second_o[0] = squares_new
        left_first = dot(ql, first_new, ((0,), (0,))).astype(jnp.bfloat16)
        first_rot = dot(left_first, qr, ((1,), (0,)))
        scaled = (first_rot / (jnp.sqrt(squares_new) + epsilon)).astype(jnp.bfloat16)
        back = dot(ql, scaled, ((1,), (0,))).astype(jnp.bfloat16)
        result = dot(back, qr, ((1,), (1,))).astype(jnp.bfloat16)
        if packed:
            halves = x_ref.shape[2]
            step = side // halves
            for h in range(halves):
                out_ref[:, 0, h] = result[h * step : (h + 1) * step].reshape(
                    x_ref.shape[0], x_ref.shape[3], side
                )
        else:
            out_ref[0] = result
        left_o[0] = (
            beta_stats * left[0].astype(jnp.float32)
            + (1.0 - beta_stats) * dot(grad, grad, ((1,), (1,)))
        ).astype(jnp.bfloat16)
        right_o[0] = (
            beta_stats * right[0].astype(jnp.float32)
            + (1.0 - beta_stats) * dot(grad, grad, ((0,), (0,)))
        ).astype(jnp.bfloat16)

    @pl.when(jnp.logical_not(used))
    def _():
        out_ref[...] = jnp.zeros_like(out_ref)
        left_o[...] = left[...]
        right_o[...] = right[...]
        moment_o[...] = moment[...]
        second_o[...] = second[...]


def precondition(x, mine, states, done, first, packed):
    left = states[0]
    slots, side, _ = left.shape
    if packed:
        dev_count, count, halves, rows, _ = x.shape
        x_spec = pl.BlockSpec((dev_count, 1, halves, rows, side), lambda i, *_: (0, i, 0, 0, 0))
    else:
        count = x.shape[0]
        x_spec = pl.BlockSpec((1, side, side), lambda i, *_: (i, 0, 0))
    state_spec = pl.BlockSpec((1, side, side), lambda i, *_: (first + i, 0, 0))
    done = list(done)
    kept = [jax.ShapeDtypeStruct(states[k].shape, states[k].dtype) for k in (0, 1, 4, 5)]
    return pl.pallas_call(
        functools.partial(slot_kernel, first, packed),
        grid_spec=pltpu.PrefetchScalarGridSpec(
            num_scalar_prefetch=1,
            grid=(count,),
            in_specs=[x_spec] + [state_spec] * 6 + [pl.BlockSpec(memory_space=pl.ANY)] * len(done),
            out_specs=[x_spec] + [state_spec] * 4,
        ),
        out_shape=[jax.ShapeDtypeStruct(x.shape, x.dtype)] + kept,
        input_output_aliases={8 + k: 1 + k for k in range(len(done))},
        cost_estimate=pl.CostEstimate(
            flops=count * 16 * side**3,
            bytes_accessed=count * side * side * 26,
            transcendentals=count * side * side,
        ),
    )(mine, x, *states, *done)


def shards(gradient, table, left_stat, right_stat, left_basis, right_basis, moment, second):
    shard_count = lax.axis_size("shard")
    tp_count = lax.axis_size("tp")
    dev_count = shard_count * tp_count
    row_dev, col_dev = gradient.shape
    slots = left_stat.shape[0]
    side = left_stat.shape[1]
    halves = side // row_dev
    cols_per_dev = col_dev // side
    block_cols = tp_count * cols_per_dev
    rows = row_dev // dev_count
    packed = rows % 16 == 0
    received = exchange(gradient.reshape(dev_count, rows, col_dev))

    state_row = slot_table(table, slots)
    block_id = table[:, 0] * block_cols + table[:, 1]
    targets = jnp.arange(dev_count * slots, dtype=jnp.int32)
    matches = (state_row[None, :] == targets[:, None]).astype(jnp.int32)
    send_id = jnp.sum(matches * block_id[None, :], axis=1)
    filled = jnp.sum(matches, axis=1)
    send_col = send_id % block_cols
    src = (send_id // block_cols) * halves * tp_count + send_col // cols_per_dev
    col = send_col % cols_per_dev
    myself = lax.axis_index(AXES)
    mine = lax.dynamic_slice_in_dim(filled, myself * slots, slots)
    positions = jnp.arange(table.shape[0], dtype=jnp.int32)
    block_match = (block_id[None, :] == positions[:, None]).astype(jnp.int32)
    slot_of_block = jnp.sum(block_match * state_row[None, :], axis=1)
    own = slot_of_block // slots
    slot = slot_of_block % slots

    half = (slots + 1) // 2
    chunks = [(0, half), (half, slots - half)] if slots > 1 else [(0, slots)]
    states = (left_stat, right_stat, left_basis, right_basis, moment, second)
    tiles = received.reshape(dev_count, rows, cols_per_dev, side)
    half_index = jnp.arange(halves, dtype=jnp.int32)
    inbox = []
    for first, count in chunks:
        if packed:
            out = pack(received, src, col, slots, first, count, halves, tp_count, side)
        else:
            src_c = src.reshape(dev_count, slots)[:, first : first + count]
            col_c = col.reshape(dev_count, slots)[:, first : first + count]
            out = tiles[src_c[:, :, None] + half_index * tp_count, :, col_c[:, :, None]]
        inbox.append(exchange(out))
    done = ()
    returned = []
    for x, (first, count) in zip(inbox, chunks):
        if not packed:
            x = x.transpose(1, 2, 0, 3, 4).reshape(count, side, side)
        update, *done = precondition(x, mine, states, done, first, packed)
        if not packed:
            update = update.reshape(count, halves, dev_count, rows, side).transpose(2, 0, 1, 3, 4)
        returned.append(exchange(update))
    if packed:
        outbox = unpack(returned, tuple(f for f, _ in chunks), own, slot, tp_count, cols_per_dev)
    else:
        back = jnp.concatenate(returned, axis=1)
        dev = jnp.arange(dev_count, dtype=jnp.int32)[:, None]
        place = (dev // tp_count // halves * tp_count + dev % tp_count) * cols_per_dev
        place = place + jnp.arange(cols_per_dev, dtype=jnp.int32)[None, :]
        picked = back[own[place], slot[place], dev // tp_count % halves]
        outbox = picked.transpose(0, 2, 1, 3).reshape(dev_count, rows, col_dev)
    update = exchange(outbox).reshape(row_dev, col_dev)
    new_left, new_right, new_moment, new_second = done
    return (update, new_left, new_right, new_moment, new_second)


def solution(mesh):
    state = P(AXES, None, None)
    in_specs = (P("shard", "tp"), P()) + (state,) * 6
    out_specs = (P("shard", "tp"),) + (state,) * 4
    return jax.shard_map(shards, mesh=mesh, in_specs=in_specs, out_specs=out_specs, check_vma=False)
```
